8 devices in a mesh: data: 8 (over z, y, x, core).
Axes of the slice: x: 2, y: 2, z: 1, core: 2. Of those that a mesh axis runs over, the one named last changes fastest.
Arguments:
- grad_qkv: bfloat16 [8, 1, 7680000], P('data')
- weight_qkv: float32 [1, 7680000], P(None, 'data')
- mom_qkv: float32 [1, 7680000], P(None, 'data')
- var_qkv: float32 [1, 7680000], P(None, 'data')
- grad_proj: bfloat16 [8, 1, 2560000], P('data')
- weight_proj: float32 [1, 2560000], P(None, 'data')
- mom_proj: float32 [1, 2560000], P(None, 'data')
- var_proj: float32 [1, 2560000], P(None, 'data')
- grad_fc_in: bfloat16 [8, 1, 10240000], P('data')
- weight_fc_in: float32 [1, 10240000], P(None, 'data')
- mom_fc_in: float32 [1, 10240000], P(None, 'data')
- var_fc_in: float32 [1, 10240000], P(None, 'data')
- grad_fc_out: bfloat16 [8, 1, 10240000], P('data')
- weight_fc_out: float32 [1, 10240000], P(None, 'data')
- mom_fc_out: float32 [1, 10240000], P(None, 'data')
- var_fc_out: float32 [1, 10240000], P(None, 'data')
Outputs:
- output 1: bfloat16 [1, 7680000], replicated
- output 2: float32 [1, 7680000], P(None, 'data')
- output 3: float32 [1, 7680000], P(None, 'data')
- output 4: float32 [1, 7680000], P(None, 'data')
- output 5: bfloat16 [1, 2560000], replicated
- output 6: float32 [1, 2560000], P(None, 'data')
- output 7: float32 [1, 2560000], P(None, 'data')
- output 8: float32 [1, 2560000], P(None, 'data')
- output 9: bfloat16 [1, 10240000], replicated
- output 10: float32 [1, 10240000], P(None, 'data')
- output 11: float32 [1, 10240000], P(None, 'data')
- output 12: float32 [1, 10240000], P(None, 'data')
- output 13: bfloat16 [1, 10240000], replicated
- output 14: float32 [1, 10240000], P(None, 'data')
- output 15: float32 [1, 10240000], P(None, 'data')
- output 16: float32 [1, 10240000], P(None, 'data')
All inputs are finite; a program needn't handle non-finite values.
Results may differ from the reference program's by a relative error of at most 0.001.
Values are sent between devices in bfloat16 or wider.
A program may use at most 1 GiB of HBM per device.

```python
import jax
import jax.numpy as jnp

D = 1600
FF = 6400
LAYERS = 1
DATA = 8
STEP = 10

LEARN_RATE = 0.1
BETA_ONE = 0.9
BETA_TWO = 0.999
EPSILON = 1e-6
WEIGHT_DECAY = 0.01
TENSOR_SHAPES = ((D, 3 * D), (D, D), (D, FF), (FF, D))
KIND_NAMES = ("qkv", "proj", "fc_in", "fc_out")


def draw_tensor(rng_key, fan_in, fan_out):
    size_flat = fan_in * fan_out
    sub_keys = jax.random.split(rng_key, 8)
    position = jnp.arange(size_flat, dtype=jnp.float32) / size_flat - 0.5
    sign_flip = 2.0 * jax.random.randint(sub_keys[0], (LAYERS, 1), 0, 2).astype(jnp.float32) - 1.0
    ramp_slope = sign_flip * jax.random.uniform(sub_keys[1], (LAYERS, 1), minval=1.0, maxval=2.0)
    weight_scale = fan_in ** -0.5 * jnp.exp(jax.random.uniform(sub_keys[2], (LAYERS, 1), minval=-1.0, maxval=1.0))
    grad_scale = 10.0 * jnp.exp(jax.random.uniform(sub_keys[3], (LAYERS, 1), minval=-1.0, maxval=1.0))
    weight = weight_scale * jnp.exp(ramp_slope * position) * jax.random.normal(sub_keys[4], (LAYERS, size_flat))
    local_grad = grad_scale * DATA ** 0.5 * jax.random.normal(sub_keys[5], (DATA, LAYERS, size_flat))
    first_mom = 0.05 * grad_scale * jax.random.normal(sub_keys[6], (LAYERS, size_flat))
    second_mom = 0.0005 * grad_scale * grad_scale * jax.random.uniform(sub_keys[7], (LAYERS, size_flat), minval=0.5, maxval=1.5)
    return local_grad.astype(jnp.bfloat16), weight, first_mom, second_mom


def setup_inputs(seed: int = 0) -> dict:
    root_key = jax.random.key(seed)
    arrays = {}
    for kind_pos in range(4):
        fan_in, fan_out = TENSOR_SHAPES[kind_pos]
        drawn_set = draw_tensor(jax.random.fold_in(root_key, kind_pos), fan_in, fan_out)
        arrays["grad_" + KIND_NAMES[kind_pos]] = drawn_set[0]
        arrays["weight_" + KIND_NAMES[kind_pos]] = drawn_set[1]
        arrays["mom_" + KIND_NAMES[kind_pos]] = drawn_set[2]
        arrays["var_" + KIND_NAMES[kind_pos]] = drawn_set[3]
    return arrays


def lamb_tensor(local_grad, weight, first_mom, second_mom):
    grad_mean = jnp.sum(local_grad, axis=0, dtype=jnp.float32) / local_grad.shape[0]
    new_first = BETA_ONE * first_mom + (1.0 - BETA_ONE) * grad_mean
    new_second = BETA_TWO * second_mom + (1.0 - BETA_TWO) * grad_mean * grad_mean
    direction = (new_first / (1.0 - BETA_ONE ** STEP)) / (jnp.sqrt(new_second / (1.0 - BETA_TWO ** STEP)) + EPSILON) + WEIGHT_DECAY * weight
    weight_norm = jnp.sqrt(jnp.sum(weight * weight, axis=1, keepdims=True))
    update_norm = jnp.sqrt(jnp.sum(direction * direction, axis=1, keepdims=True))
    new_weight = weight - LEARN_RATE * (weight_norm / update_norm) * direction
    return new_weight.astype(jnp.bfloat16), new_weight, new_first, new_second


def reference(grad_qkv, weight_qkv, mom_qkv, var_qkv, grad_proj, weight_proj, mom_proj, var_proj, grad_fc_in, weight_fc_in, mom_fc_in, var_fc_in, grad_fc_out, weight_fc_out, mom_fc_out, var_fc_out):
    copy_qkv, new_weight_qkv, new_mom_qkv, new_var_qkv = lamb_tensor(grad_qkv, weight_qkv, mom_qkv, var_qkv)
    copy_proj, new_weight_proj, new_mom_proj, new_var_proj = lamb_tensor(grad_proj, weight_proj, mom_proj, var_proj)
    copy_fc_in, new_weight_fc_in, new_mom_fc_in, new_var_fc_in = lamb_tensor(grad_fc_in, weight_fc_in, mom_fc_in, var_fc_in)
    copy_fc_out, new_weight_fc_out, new_mom_fc_out, new_var_fc_out = lamb_tensor(grad_fc_out, weight_fc_out, mom_fc_out, var_fc_out)
    return (copy_qkv, new_weight_qkv, new_mom_qkv, new_var_qkv, copy_proj, new_weight_proj, new_mom_proj, new_var_proj, copy_fc_in, new_weight_fc_in, new_mom_fc_in, new_var_fc_in, copy_fc_out, new_weight_fc_out, new_mom_fc_out, new_var_fc_out)
```

```python
import functools

import jax
import jax.numpy as jnp
from jax import lax
from jax.experimental import pallas as pl
from jax.experimental.pallas import tpu as pltpu
from jax.sharding import PartitionSpec as P

STEP = 10
LEARN_RATE = 0.1
BETA_ONE = 0.9
BETA_TWO = 0.999
EPSILON = 1e-6
WEIGHT_DECAY = 0.01

LANES = 128
TILE = 8 * LANES
VMEM_BYTES = 48 * 1024 * 1024


def splits(total, unit, most):
    units = total // unit
    best = max(d for d in range(1, most + 1) if d <= max(units, 1))
    for d in range(best, 0, -1):
        if units - (units // d) * d <= 0:
            best = d
            break
    steps = units // best
    return steps, best * unit, total - steps * best * unit


def over(total, unit, most, body, carry=0):
    steps, length, rest = splits(total, unit, most)
    carry = lax.fori_loop(0, steps, lambda i, c: body(pl.multiple_of(i * length, unit), length, c), carry)
    if rest:
        carry = body(steps * length, rest, carry)
    return carry


def params():
    return pltpu.CompilerParams(vmem_limit_bytes=VMEM_BYTES)


def cost(elements, flops, total_bytes):
    return pl.CostEstimate(flops=int(elements * flops), bytes_accessed=int(total_bytes), transcendentals=0)


class Tensor:
    def __init__(self, n, parts):
        self.n, self.parts = n, parts
        self.shard = n // 8
        self.block = self.shard // parts
        self.rows = self.block // LANES

    def grad_spec(self, owner):
        return pl.BlockSpec((None, 1, self.block), lambda i, s: (0, 0, s[owner] * self.parts + i))

    def flat_spec(self):
        return pl.BlockSpec((1, self.block), lambda i, s: (0, i))

    def flat_shape(self):
        return jax.ShapeDtypeStruct((1, self.shard), jnp.float32)

    def call(self, kernel, operands, in_specs, out_specs, out_shape, scratch=(), aliases=None, flops=4, moved=12, name=None, grid=None):
        return pl.pallas_call(
            kernel,
            name=name,
            out_shape=out_shape,
            grid_spec=pltpu.PrefetchScalarGridSpec(
                num_scalar_prefetch=1, grid=grid or (self.parts,), in_specs=in_specs, out_specs=out_specs, scratch_shapes=scratch
            ),
            input_output_aliases=aliases or {},
            compiler_params=params(),
            cost_estimate=cost(self.shard, flops, self.shard * moved),
        )(*operands)

    def pair_sum(self, owners, grad, other, owner, received=None):
        def kernel(s, *refs):
            *ins, out = refs

            def step(start, length, c):
                at = (slice(None), pl.ds(start, length))
                total = ins[0][at].astype(jnp.float32) + ins[1][at].astype(jnp.float32)
                if received is not None:
                    total = total + ins[2][at]
                out[at] = total
                return c

            over(self.block, TILE, 25, step)

        more = [] if received is None else [received]
        return self.call(
            kernel,
            [owners, grad, other, *more],
            [self.grad_spec(owner), self.grad_spec(owner)] + [self.flat_spec()] * len(more),
            self.flat_spec(),
            self.flat_shape(),
            moved=12 + 4 * len(more),
            name="pair_sum",
        )

    def moments(self, owners, grad, other, first, second, weight, first_mom, second_mom):
        def kernel(s, g, h, f, t, w, m, v, new_m, new_v, dirn, sums, acc):
            @pl.when(pl.program_id(0) == 0)
            def _():
                acc[0] = 0.0
                acc[1] = 0.0

            def step(start, length, c):
                at = (slice(None), pl.ds(start, length))
                total = (g[at].astype(jnp.float32) + h[at].astype(jnp.float32)) + f[at] + t[at]
                mean = total / 8
                nm = BETA_ONE * m[at] + (1.0 - BETA_ONE) * mean
                nv = BETA_TWO * v[at] + (1.0 - BETA_TWO) * mean * mean
                new_m[at] = nm
                new_v[at] = nv
                wt = w[at]
                u = (nm / (1.0 - BETA_ONE**STEP)) / (jnp.sqrt(nv / (1.0 - BETA_TWO**STEP)) + EPSILON) + WEIGHT_DECAY * wt
                dirn[at] = u
                return c[0] + jnp.sum(wt * wt), c[1] + jnp.sum(u * u)

            a, b = over(self.block, TILE, 25, step, (jnp.float32(0), jnp.float32(0)))
            acc[0] += a
            acc[1] += b

            @pl.when(pl.program_id(0) == self.parts - 1)
            def _():
                lane = lax.broadcasted_iota(jnp.int32, (1, LANES), 1)
                sums[...] = jnp.where(lane == 0, acc[0], acc[1])

        return self.call(
            kernel,
            [owners, grad, other, first, second, weight, first_mom, second_mom],
            [self.grad_spec(0), self.grad_spec(0)] + [self.flat_spec()] * 5,
            [self.flat_spec()] * 3 + [pl.BlockSpec((1, LANES), lambda i, s: (0, 0))],
            [self.flat_shape()] * 3 + [jax.ShapeDtypeStruct((1, LANES), jnp.float32)],
            scratch=[pltpu.SMEM((2,), jnp.float32)],
            flops=30,
            moved=40,
            name="moments",
        )

    def apply(self, owners, sums, weight, dirn):
        def kernel(s, p, w, u, new_w, packed):
            norms = jnp.sqrt(p[...])
            scale = LEARN_RATE * (norms[:, 0:1] / norms[:, 1:2])

            def step(start, length, c):
                row0 = pl.multiple_of(start, 16)
                at = (slice(None), pl.ds(pl.multiple_of(start * LANES, LANES), length * LANES))
                nw = w[at] - scale * u[at]
                new_w[at] = nw
                packed[pl.ds(row0, length), :] = nw.reshape(length, LANES).astype(jnp.bfloat16)
                return c

            over(self.rows, 16, 16, step)

        return self.call(
            kernel,
            [owners, sums, weight, dirn],
            [pl.BlockSpec((1, LANES), lambda i, s: (0, 0)), self.flat_spec(), self.flat_spec()],
            [self.flat_spec(), self.packed_spec()],
            [self.flat_shape(), jax.ShapeDtypeStruct((self.parts, self.rows, LANES), jnp.bfloat16)],
            moved=14,
            name="apply",
        )

    def packed_spec(self):
        return pl.BlockSpec((None, self.rows, LANES), lambda i, s: (i, 0, 0))

    def unpack(self, owners, owner, mine, theirs, whole):
        def kernel(s, a, b, *refs):
            out = refs[-1]

            def put(src):
                def step(start, length, c):
                    at = (slice(None), pl.ds(pl.multiple_of(start * LANES, LANES), length * LANES))
                    piece = src[pl.ds(pl.multiple_of(start, 16), length), :].astype(jnp.float32)
                    out[at] = piece.reshape(1, length * LANES).astype(jnp.bfloat16)
                    return c

                over(self.rows, 16, 16, step)

            @pl.when(pl.program_id(0) < self.parts)
            def _():
                put(a)

            @pl.when(pl.program_id(0) >= self.parts)
            def _():
                put(b)

        parts = self.parts
        out_spec = pl.BlockSpec(
            (1, self.block), lambda i, s: (0, jnp.where(i < parts, s[owner], s[owner + 4]) * parts + lax.rem(i, parts))
        )
        more = [] if whole is None else [whole]
        return self.call(
            kernel,
            [owners, mine, theirs, *more],
            [
                pl.BlockSpec((None, self.rows, LANES), lambda i, s: (jnp.minimum(i, parts - 1), 0, 0)),
                pl.BlockSpec((None, self.rows, LANES), lambda i, s: (jnp.maximum(i - parts, 0), 0, 0)),
            ]
            + [pl.BlockSpec(memory_space=pl.ANY)] * len(more),
            out_spec,
            jax.ShapeDtypeStruct((1, self.n), jnp.bfloat16),
            aliases={3: 0} if more else None,
            moved=12,
            name="unpack",
            grid=(2 * parts,),
        )


def solution(mesh):
    grad_spec = P("data", None, None)
    shard_spec = P(None, "data")
    full_spec = P(None, None)

    core_perm = [(i, i ^ 1) for i in range(8)]
    first_perm = [(i, i ^ (2 if i % 2 == 0 else 4)) for i in range(8)]
    second_perm = [(i, i ^ (4 if i % 2 == 0 else 2)) for i in range(8)]

    def send(value, perm):
        return lax.ppermute(value, "data", perm)

    def total(sums):
        for perm in (core_perm, first_perm, second_perm):
            sums = sums + send(sums, perm)
        return sums

    def device_step(*blocks):
        me = lax.axis_index("data")
        core = lax.rem(me, 2)
        first = jnp.where(core == 0, me ^ 2, me ^ 4)
        second = jnp.where(core == 0, me ^ 4, me ^ 2)
        owners = jnp.stack([me, first, second, me ^ 6, me ^ 1, second ^ 1, first ^ 1, me ^ 7]).astype(jnp.int32)
        kinds = {}
        for pos in range(4):
            grad, weight, first_mom, second_mom = blocks[4 * pos : 4 * pos + 4]
            n = grad.shape[2]
            kinds[pos] = (Tensor(n, 5), grad, weight, first_mom, second_mom)
        others, states, results = {}, {}, {}
        order = [1, 2, 3, 0]
        for pos in order:
            others[pos] = send(kinds[pos][1], core_perm)
        for pos in order:
            tensor, grad, weight, first_mom, second_mom = kinds[pos]
            other = others[pos]
            far = send(tensor.pair_sum(owners, grad, other, 3), first_perm)
            near = send(tensor.pair_sum(owners, grad, other, 1), first_perm)
            turn = send(tensor.pair_sum(owners, grad, other, 2, far), second_perm)
            new_m, new_v, dirn, sums = tensor.moments(owners, grad, other, near, turn, weight, first_mom, second_mom)
            states[pos] = (new_m, new_v, dirn, total(sums))
        for pos in [2, 3, 0, 1]:
            tensor, grad, weight, first_mom, second_mom = kinds[pos]
            new_m, new_v, dirn, sums = states[pos]
            new_w, packed = tensor.apply(owners, sums, weight, dirn)
            by_second = send(packed, second_perm)
            by_first = send(packed, first_perm)
            by_both = send(by_second, first_perm)
            whole = None
            for owner, part in ((0, packed), (2, by_second), (1, by_first), (3, by_both)):
                whole = tensor.unpack(owners, owner, part, send(part, core_perm), whole)
            results[pos] = (whole, new_w, new_m, new_v)
        return tuple(value for pos in range(4) for value in results[pos])

    return jax.shard_map(
        device_step,
        mesh=mesh,
        in_specs=(grad_spec, shard_spec, shard_spec, shard_spec) * 4,
        out_specs=(full_spec, shard_spec, shard_spec, shard_spec) * 4,
        check_vma=False,
    )
```

```python
import jax
import jax.numpy as jnp
from jax import lax
from jax.experimental import pallas as pl
from jax.experimental.pallas import tpu as pltpu
from jax.sharding import PartitionSpec as P

STEP = 10
LEARN_RATE = 0.1
BETA_ONE = 0.9
BETA_TWO = 0.999
EPSILON = 1e-6
WEIGHT_DECAY = 0.01

LANES = 128
TILE = 8 * LANES
VMEM_BYTES = 66900000
KINDS = ("q", "p", "i", "o")
SPLIT = ("q_u3",)
STEPS = {"q": (2, 2), "p": (2, 1), "i": (2, 2), "o": (2, 2)}


def over(total, unit, most, body, carry=0):
    length = unit * min(most, max(total // unit, 1))
    steps = total // length
    carry = lax.fori_loop(0, steps, lambda i, c: body(pl.multiple_of(i * length, unit), length, c), carry)
    if total - steps * length:
        carry = body(steps * length, total - steps * length, carry)
    return carry


def folded(values):
    length = values.shape[1]
    whole = length // TILE * TILE
    parts = [jnp.sum(values[:, :whole].reshape(whole // TILE, 8, LANES), axis=0)]
    for start in range(whole, length, LANES):
        piece = values[:, start : start + LANES]
        parts.append(jnp.concatenate([piece, jnp.zeros((7, LANES), jnp.float32)], axis=0))
    return sum(parts[1:], parts[0])


def params():
    return pltpu.CompilerParams(vmem_limit_bytes=VMEM_BYTES)


def cost(elements, flops, total_bytes):
    return pl.CostEstimate(flops=int(elements * flops), bytes_accessed=int(total_bytes), transcendentals=0)


TURNS = ((0, 0), (2, 4), (4, 2), (6, 6), (1, 1), (5, 3), (3, 5), (7, 7))


def index_of(place):
    me = lax.axis_index("data")
    zero, one = TURNS[place]
    return me ^ zero if zero == one else jnp.where(lax.rem(me, 2) == 0, me ^ zero, me ^ one)


def among(places, i, parts):
    owner = index_of(places[0])
    for k in range(1, len(places)):
        owner = jnp.where(i >= k * parts, index_of(places[k]), owner)
    return owner


class Tensor:
    def __init__(self, n, parts):
        self.n, self.parts = n, parts
        self.shard = n // 8
        self.block = self.shard // parts

    def grad_spec(self, owner):
        return pl.BlockSpec((None, 1, self.block), lambda i: (0, 0, index_of(owner) * self.parts + i))

    def flat_spec(self):
        return pl.BlockSpec((1, self.block), lambda i: (0, i))

    def flat_shape(self):
        return jax.ShapeDtypeStruct((1, self.shard), jnp.float32)

    def call(self, kernel, operands, in_specs, out_specs, out_shape, scratch=(), aliases=None, flops=4, moved=12, grid=None):
        return pl.pallas_call(
            kernel,
            out_shape=out_shape,
            grid=grid or (self.parts,),
            in_specs=in_specs,
            out_specs=out_specs,
            scratch_shapes=scratch,
            input_output_aliases=aliases or {},
            compiler_params=params(),
            cost_estimate=cost(self.shard, flops, self.shard * moved),
        )(*operands)

    def other_spec(self, place):
        skip = place * self.parts
        return pl.BlockSpec((None, 1, self.block), lambda i: (0, 0, skip + i))

    def extract(self, grad, places):
        def kernel(g, out):
            def step(start, length, c):
                at = (slice(None), pl.ds(start, length))
                out[at] = g[at]
                return c

            over(self.block, TILE, 25, step)

        parts = self.parts

        def source(i):
            return (0, 0, among(places, i, parts) * parts + lax.rem(i, parts))

        return self.call(
            kernel,
            [grad],
            [pl.BlockSpec((None, 1, self.block), source)],
            pl.BlockSpec((None, 1, self.block), lambda i: (0, 0, i)),
            jax.ShapeDtypeStruct((1, 1, len(places) * self.shard), jnp.bfloat16),
            moved=8 * len(places),
            grid=(len(places) * parts,),
        )

    def halves(self, grad, owner):
        half = self.block // 2

        def kernel(src, out):
            def step(start, length, c):
                rows = [src[:, pl.ds(pl.multiple_of(start + skip, LANES), length)].astype(jnp.float32) for skip in (0, half)]
                out[:, pl.ds(start, length)] = jnp.concatenate(rows, axis=0).astype(jnp.bfloat16)
                return c

            over(half, TILE, 16, step)

        return self.call(
            kernel,
            [grad],
            [self.grad_spec(owner)],
            self.packed_spec(),
            jax.ShapeDtypeStruct((2, self.shard // 2), jnp.bfloat16),
            moved=6,
        )

    def sum_steps(self, raws, body, carry=0):
        if not raws:
            return over(self.block, TILE, 25, lambda start, length, c: body((slice(None), pl.ds(start, length)), None, c), carry)
        half = self.block // 2

        def step(start, length, c):
            for row in range(2):
                at = (slice(None), pl.ds(pl.multiple_of(start + row * half, LANES), length))
                pieces = [raw[row : row + 1, pl.ds(start, length)].astype(jnp.float32) for raw in raws]
                c = body(at, pieces[0] + pieces[1], c)
            return c

        return over(half, TILE, 16, step, carry)

    def pair_sum(self, grad, other, owner, place, received=None, raws=()):
        def kernel(*refs):
            *ins, out = refs
            raw_refs = ins[len(ins) - len(raws) :]

            def step(at, raw, c):
                total = ins[0][at].astype(jnp.float32) + ins[1][at].astype(jnp.float32)
                if received is not None:
                    total = total + ins[2][at]
                if raw is not None:
                    total = total + raw
                out[at] = total
                return c

            self.sum_steps(raw_refs if raws else (), step)

        more = [] if received is None else [received]
        return self.call(
            kernel,
            [grad, other, *more, *raws],
            [self.grad_spec(owner), self.other_spec(place)] + [self.flat_spec()] * len(more) + [self.packed_spec()] * len(raws),
            self.flat_spec(),
            self.flat_shape(),
            moved=12 + 4 * len(more),
        )

    def moments(self, grad, other, near, turn, weight, first_mom, second_mom, raws=()):
        given = [value for value in (near, turn, weight, first_mom, second_mom) if value is not None]

        def kernel(g, h, *refs):
            ins, raw_refs = refs[: len(given)], refs[len(given) : len(given) + len(raws)]
            new_m, new_v, dirn, sums, acc = refs[len(given) + len(raws) :]
            t, w, m, v = ins[-4:]

            @pl.when(pl.program_id(0) == 0)
            def _():
                acc[...] = jnp.zeros_like(acc)

            def step(at, raw, c):
                total = (g[at].astype(jnp.float32) + h[at].astype(jnp.float32)) + (ins[0][at] if raw is None else raw) + t[at]
                mean = total / 8
                nm = BETA_ONE * m[at] + (1.0 - BETA_ONE) * mean
                nv = BETA_TWO * v[at] + (1.0 - BETA_TWO) * mean * mean
                new_m[at] = nm
                new_v[at] = nv
                wt = w[at]
                u = (nm / (1.0 - BETA_ONE**STEP)) / (jnp.sqrt(nv / (1.0 - BETA_TWO**STEP)) + EPSILON) + WEIGHT_DECAY * wt
                dirn[at] = u
                return c[0] + folded(wt * wt), c[1] + folded(u * u)

            a, b = self.sum_steps(raw_refs, step, (acc[0], acc[1]))
            acc[0] = a
            acc[1] = b

            @pl.when(pl.program_id(0) == self.parts - 1)
            def _():
                lane = lax.broadcasted_iota(jnp.int32, (1, LANES), 1)
                sums[...] = jnp.where(lane == 0, jnp.sum(a), jnp.sum(b))

        return self.call(
            kernel,
            [grad, other, *given, *raws],
            [self.grad_spec(0), self.other_spec(0)] + [self.flat_spec()] * len(given) + [self.packed_spec()] * len(raws),
            [self.flat_spec()] * 3 + [pl.BlockSpec((1, LANES), lambda i: (0, 0))],
            [self.flat_shape()] * 3 + [jax.ShapeDtypeStruct((1, LANES), jnp.float32)],
            scratch=[pltpu.VMEM((2, 8, LANES), jnp.float32)],
            flops=30,
            moved=40,
        )

    def apply(self, sums, weight, dirn):
        def kernel(p, w, u, new_w, packed):
            norms = jnp.sqrt(p[...])
            scale = LEARN_RATE * (norms[:, 0:1] / norms[:, 1:2])

            half = self.block // 2

            def step(start, length, c):
                ats = [(slice(None), pl.ds(pl.multiple_of(start + skip, LANES), length)) for skip in (0, half)]
                news = [w[at] - scale * u[at] for at in ats]
                for at, new in zip(ats, news):
                    new_w[at] = new
                packed[ats[0]] = jnp.concatenate(news, axis=0).astype(jnp.bfloat16)
                return c

            over(half, TILE, 16, step)

        return self.call(
            kernel,
            [sums, weight, dirn],
            [pl.BlockSpec((1, LANES), lambda i: (0, 0)), self.flat_spec(), self.flat_spec()],
            [self.flat_spec(), self.packed_spec()],
            [self.flat_shape(), jax.ShapeDtypeStruct((2, self.shard // 2), jnp.bfloat16)],
            moved=14,
        )

    def packed_spec(self):
        return pl.BlockSpec((2, self.block // 2), lambda i: (0, i))

    def unpack(self, pieces, whole):
        parts, half = self.parts, self.block // 2
        places, arrays = zip(*pieces)

        def kernel(*refs):
            out = refs[-1]

            def put(src):
                def step(start, length, c):
                    for row in range(2):
                        to = pl.ds(pl.multiple_of(start + row * half, LANES), length)
                        out[:, to] = src[row : row + 1, pl.ds(start, length)]
                    return c

                over(half, TILE, 16, step)

            for k in range(len(arrays)):
                pl.when(lax.div(pl.program_id(0), parts) == k)(lambda src=refs[k]: put(src))

        def source(k):
            return pl.BlockSpec((2, half), lambda i: (0, jnp.clip(i - k * parts, 0, parts - 1)))

        def target(i):
            return (0, among(places, i, parts) * parts + lax.rem(i, parts))

        more = [] if whole is None else [whole]
        return self.call(
            kernel,
            [*arrays, *more],
            [source(k) for k in range(len(arrays))] + [pl.BlockSpec(memory_space=pl.ANY)] * len(more),
            pl.BlockSpec((1, self.block), target),
            jax.ShapeDtypeStruct((1, self.n), jnp.bfloat16),
            aliases={len(arrays): 0} if more else None,
            moved=6 * len(arrays),
            grid=(len(arrays) * parts,),
        )


def solution(mesh):
    grad_spec = P("data", None, None)
    shard_spec = P(None, "data")
    full_spec = P(None, None)

    core_perm = [(i, i ^ 1) for i in range(8)]
    first_perm = [(i, i ^ (2 if i % 2 == 0 else 4)) for i in range(8)]
    second_perm = [(i, i ^ (4 if i % 2 == 0 else 2)) for i in range(8)]

    both_perm = [(i, i ^ 6) for i in range(8)]
    cross_perm = [(i, i ^ (5 if i % 2 == 0 else 3)) for i in range(8)]

    def send(value, perm):
        return lax.ppermute(value, "data", perm)

    def device_step(*blocks):
        results = []
        for pos, k in enumerate(KINDS):
            grad, weight, first_mom, second_mom = blocks[4 * pos : 4 * pos + 4]
            tensor = Tensor(grad.shape[2], STEPS[k][0])
            copies = Tensor(grad.shape[2], STEPS[k][1])
            state = (weight, first_mom, second_mom)
            if k == "p":
                far, near = (
                    (send(tensor.halves(grad, place), first_perm), send(tensor.halves(grad, place + 4), cross_perm))
                    for place in (3, 1)
                )
                other = send(tensor.extract(grad, (4, 6)), core_perm)
                turn = send(tensor.pair_sum(grad, other, 2, 1, None, far), second_perm)
                new_m, new_v, dirn, sums = tensor.moments(grad, other, None, turn, *state, near)
            else:
                other_far = send(tensor.extract(grad, (7,)), core_perm)
                other = send(tensor.extract(grad, (4, 5, 6)), core_perm)
                far = send(tensor.pair_sum(grad, other_far, 3, 0), first_perm)
                near = send(tensor.pair_sum(grad, other, 1, 1), first_perm)
                turn = send(tensor.pair_sum(grad, other, 2, 2, far), second_perm)
                new_m, new_v, dirn, sums = tensor.moments(grad, other, near, turn, *state)
            sums = sums + send(sums, core_perm)
            sums = (sums + send(sums, both_perm)) + (send(sums, first_perm) + send(sums, second_perm))
            new_w, packed = copies.apply(sums, weight, dirn)
            by_second = send(packed, second_perm)
            by_first = send(packed, first_perm)
            by_both = send(by_second, first_perm)
            whole = None
            for owner, part in ((0, packed), (2, by_second), (1, by_first), (3, by_both)):
                name = k + "_u" + str(owner)
                pieces = ((owner, part), (owner + 4, send(part, core_perm)))
                if name in SPLIT:
                    whole = copies.unpack(pieces[:1], whole)
                    whole = copies.unpack(pieces[1:], whole)
                else:
                    whole = copies.unpack(pieces, whole)
            results.extend((whole, new_w, new_m, new_v))
        return tuple(results)

    return jax.shard_map(
        device_step,
        mesh=mesh,
        in_specs=(grad_spec, shard_spec, shard_spec, shard_spec) * 4,
        out_specs=(full_spec, shard_spec, shard_spec, shard_spec) * 4,
        check_vma=False,
    )
```

```python
import jax
import jax.numpy as jnp
from jax import lax
from jax.experimental import pallas as pl
from jax.experimental.pallas import tpu as pltpu
from jax.sharding import PartitionSpec as P

STEP = 10
LEARN_RATE = 0.1
BETA_ONE = 0.9
BETA_TWO = 0.999
EPSILON = 1e-6
WEIGHT_DECAY = 0.01

LANES = 128
TILE = 8 * LANES
VMEM_BYTES = 63000000
KINDS = ("q", "p", "i", "o")
STEPS = {"q": (5, 2), "p": (2, 2), "i": (5, 2), "o": (5, 2)}


def over(total, unit, most, body, carry=0):
    length = unit * min(most, max(total // unit, 1))
    steps = total // length
    carry = lax.fori_loop(0, steps, lambda i, c: body(pl.multiple_of(i * length, unit), length, c), carry)
    if total - steps * length:
        carry = body(steps * length, total - steps * length, carry)
    return carry


def folded(values):
    length = values.shape[1]
    whole = length // TILE * TILE
    parts = [jnp.sum(values[:, :whole].reshape(whole // TILE, 8, LANES), axis=0)]
    for start in range(whole, length, LANES):
        piece = values[:, start : start + LANES]
        parts.append(jnp.concatenate([piece, jnp.zeros((7, LANES), jnp.float32)], axis=0))
    return sum(parts[1:], parts[0])


def params():
    return pltpu.CompilerParams(vmem_limit_bytes=VMEM_BYTES)


def cost(elements, flops, total_bytes):
    return pl.CostEstimate(flops=int(elements * flops), bytes_accessed=int(total_bytes), transcendentals=0)


class Tensor:
    def __init__(self, n, parts):
        self.n, self.parts = n, parts
        self.shard = n // 8
        self.block = self.shard // parts

    def grad_spec(self, owner):
        return pl.BlockSpec((None, 1, self.block), lambda i, s: (0, 0, s[owner] * self.parts + i))

    def flat_spec(self):
        return pl.BlockSpec((1, self.block), lambda i, s: (0, i))

    def flat_shape(self):
        return jax.ShapeDtypeStruct((1, self.shard), jnp.float32)

    def call(self, kernel, operands, in_specs, out_specs, out_shape, scratch=(), aliases=None, flops=4, moved=12, grid=None):
        return pl.pallas_call(
            kernel,
            out_shape=out_shape,
            grid_spec=pltpu.PrefetchScalarGridSpec(
                num_scalar_prefetch=1, grid=grid or (self.parts,), in_specs=in_specs, out_specs=out_specs, scratch_shapes=scratch
            ),
            input_output_aliases=aliases or {},
            compiler_params=params(),
            cost_estimate=cost(self.shard, flops, self.shard * moved),
        )(*operands)

    def other_spec(self, place):
        skip = place * self.parts
        return pl.BlockSpec((None, 1, self.block), lambda i, s: (0, 0, skip + i))

    def extract(self, owners, grad, places):
        def kernel(s, g, out):
            def step(start, length, c):
                at = (slice(None), pl.ds(start, length))
                out[at] = g[at]
                return c

            over(self.block, TILE, 25, step)

        parts = self.parts
        stride = places[1] - places[0] if len(places) > 1 else 1

        def source(i, s):
            return (0, 0, s[places[0] + stride * lax.div(i, parts)] * parts + lax.rem(i, parts))

        return self.call(
            kernel,
            [owners, grad],
            [pl.BlockSpec((None, 1, self.block), source)],
            pl.BlockSpec((None, 1, self.block), lambda i, s: (0, 0, i)),
            jax.ShapeDtypeStruct((1, 1, len(places) * self.shard), jnp.bfloat16),
            moved=8 * len(places),
            grid=(len(places) * parts,),
        )

    def halves(self, owners, grad, places):
        half = self.block // 2
        count = len(places)

        def kernel(s, *refs):
            def step(start, length, c):
                for src, out in zip(refs[:count], refs[count:]):
                    rows = [src[:, pl.ds(pl.multiple_of(start + skip, LANES), length)].astype(jnp.float32) for skip in (0, half)]
                    out[:, pl.ds(start, length)] = jnp.concatenate(rows, axis=0).astype(jnp.bfloat16)
                return c

            over(half, TILE, 16, step)

        return self.call(
            kernel,
            [owners] + [grad] * count,
            [self.grad_spec(place) for place in places],
            [self.packed_spec()] * count,
            [jax.ShapeDtypeStruct((2, self.shard // 2), jnp.bfloat16)] * count,
            moved=6 * count,
        )

    def sum_steps(self, raws, body, carry=0):
        if not raws:
            return over(self.block, TILE, 25, lambda start, length, c: body((slice(None), pl.ds(start, length)), None, c), carry)
        half = self.block // 2

        def step(start, length, c):
            for row in range(2):
                at = (slice(None), pl.ds(pl.multiple_of(start + row * half, LANES), length))
                pieces = [raw[row : row + 1, pl.ds(start, length)].astype(jnp.float32) for raw in raws]
                c = body(at, pieces[0] + pieces[1], c)
            return c

        return over(half, TILE, 16, step, carry)

    def pair_sum(self, owners, grad, other, owner, place, received=None, raws=()):
        def kernel(s, *refs):
            *ins, out = refs
            raw_refs = ins[len(ins) - len(raws) :]

            def step(at, raw, c):
                total = ins[0][at].astype(jnp.float32) + ins[1][at].astype(jnp.float32)
                if received is not None:
                    total = total + ins[2][at]
                if raw is not None:
                    total = total + raw
                out[at] = total
                return c

            self.sum_steps(raw_refs if raws else (), step)

        more = [] if received is None else [received]
        return self.call(
            kernel,
            [owners, grad, other, *more, *raws],
            [self.grad_spec(owner), self.other_spec(place)] + [self.flat_spec()] * len(more) + [self.packed_spec()] * len(raws),
            self.flat_spec(),
            self.flat_shape(),
            moved=12 + 4 * len(more),
        )

    def moments(self, owners, grad, other, near, turn, weight, first_mom, second_mom, raws=()):
        given = [value for value in (near, turn, weight, first_mom, second_mom) if value is not None]

        def kernel(s, g, h, *refs):
            ins, raw_refs = refs[: len(given)], refs[len(given) : len(given) + len(raws)]
            new_m, new_v, dirn, sums, acc = refs[len(given) + len(raws) :]
            t, w, m, v = ins[-4:]

            @pl.when(pl.program_id(0) == 0)
            def _():
                acc[...] = jnp.zeros_like(acc)

            def step(at, raw, c):
                total = (g[at].astype(jnp.float32) + h[at].astype(jnp.float32)) + (ins[0][at] if raw is None else raw) + t[at]
                mean = total / 8
                nm = BETA_ONE * m[at] + (1.0 - BETA_ONE) * mean
                nv = BETA_TWO * v[at] + (1.0 - BETA_TWO) * mean * mean
                new_m[at] = nm
                new_v[at] = nv
                wt = w[at]
                u = (nm / (1.0 - BETA_ONE**STEP)) / (jnp.sqrt(nv / (1.0 - BETA_TWO**STEP)) + EPSILON) + WEIGHT_DECAY * wt
                dirn[at] = u
                return c[0] + folded(wt * wt), c[1] + folded(u * u)

            a, b = self.sum_steps(raw_refs, step, (acc[0], acc[1]))
            acc[0] = a
            acc[1] = b

            @pl.when(pl.program_id(0) == self.parts - 1)
            def _():
                lane = lax.broadcasted_iota(jnp.int32, (1, LANES), 1)
                sums[...] = jnp.where(lane == 0, jnp.sum(a), jnp.sum(b))

        return self.call(
            kernel,
            [owners, grad, other, *given, *raws],
            [self.grad_spec(0), self.other_spec(0)] + [self.flat_spec()] * len(given) + [self.packed_spec()] * len(raws),
            [self.flat_spec()] * 3 + [pl.BlockSpec((1, LANES), lambda i, s: (0, 0))],
            [self.flat_shape()] * 3 + [jax.ShapeDtypeStruct((1, LANES), jnp.float32)],
            scratch=[pltpu.VMEM((2, 8, LANES), jnp.float32)],
            flops=30,
            moved=40,
        )

    def apply(self, owners, sums, weight, dirn):
        def kernel(s, p, w, u, new_w, packed):
            norms = jnp.sqrt(p[...])
            scale = LEARN_RATE * (norms[:, 0:1] / norms[:, 1:2])

            half = self.block // 2

            def step(start, length, c):
                ats = [(slice(None), pl.ds(pl.multiple_of(start + skip, LANES), length)) for skip in (0, half)]
                news = [w[at] - scale * u[at] for at in ats]
                for at, new in zip(ats, news):
                    new_w[at] = new
                packed[ats[0]] = jnp.concatenate(news, axis=0).astype(jnp.bfloat16)
                return c

            over(half, TILE, 16, step)

        return self.call(
            kernel,
            [owners, sums, weight, dirn],
            [pl.BlockSpec((1, LANES), lambda i, s: (0, 0)), self.flat_spec(), self.flat_spec()],
            [self.flat_spec(), self.packed_spec()],
            [self.flat_shape(), jax.ShapeDtypeStruct((2, self.shard // 2), jnp.bfloat16)],
            moved=14,
        )

    def packed_spec(self):
        return pl.BlockSpec((2, self.block // 2), lambda i, s: (0, i))

    def unpack(self, owners, owner, mine, theirs, whole):
        def kernel(s, a, b, *refs):
            out = refs[-1]

            half = self.block // 2

            def put(src):
                def step(start, length, c):
                    for row in range(2):
                        to = pl.ds(pl.multiple_of(start + row * half, LANES), length)
                        out[:, to] = src[row : row + 1, pl.ds(start, length)]
                    return c

                over(half, TILE, 16, step)

            @pl.when(pl.program_id(0) < self.parts)
            def _():
                put(a)

            @pl.when(pl.program_id(0) >= self.parts)
            def _():
                put(b)

        parts = self.parts
        out_spec = pl.BlockSpec(
            (1, self.block), lambda i, s: (0, jnp.where(i < parts, s[owner], s[owner + 4]) * parts + lax.rem(i, parts))
        )
        more = [] if whole is None else [whole]
        return self.call(
            kernel,
            [owners, mine, theirs, *more],
            [
                pl.BlockSpec((2, self.block // 2), lambda i, s: (0, jnp.minimum(i, parts - 1))),
                pl.BlockSpec((2, self.block // 2), lambda i, s: (0, jnp.maximum(i - parts, 0))),
            ]
            + [pl.BlockSpec(memory_space=pl.ANY)] * len(more),
            out_spec,
            jax.ShapeDtypeStruct((1, self.n), jnp.bfloat16),
            aliases={3: 0} if more else None,
            moved=12,
            grid=(2 * parts,),
        )


def solution(mesh):
    grad_spec = P("data", None, None)
    shard_spec = P(None, "data")
    full_spec = P(None, None)

    core_perm = [(i, i ^ 1) for i in range(8)]
    first_perm = [(i, i ^ (2 if i % 2 == 0 else 4)) for i in range(8)]
    second_perm = [(i, i ^ (4 if i % 2 == 0 else 2)) for i in range(8)]

    both_perm = [(i, i ^ 6) for i in range(8)]
    cross_perm = [(i, i ^ (5 if i % 2 == 0 else 3)) for i in range(8)]

    def send(value, perm):
        return lax.ppermute(value, "data", perm)

    def device_step(*blocks):
        me = lax.axis_index("data")
        core = lax.rem(me, 2)
        first = jnp.where(core == 0, me ^ 2, me ^ 4)
        second = jnp.where(core == 0, me ^ 4, me ^ 2)
        owners = jnp.stack([me, first, second, me ^ 6, me ^ 1, second ^ 1, first ^ 1, me ^ 7]).astype(jnp.int32)
        results = []
        for pos, k in enumerate(KINDS):
            grad, weight, first_mom, second_mom = blocks[4 * pos : 4 * pos + 4]
            tensor = Tensor(grad.shape[2], STEPS[k][0])
            copies = Tensor(grad.shape[2], STEPS[k][1])
            state = (weight, first_mom, second_mom)
            if k == "p":
                ours, cross = tensor.halves(owners, grad, (3, 7))
                far = (send(ours, first_perm), send(cross, cross_perm))
                ours, cross = tensor.halves(owners, grad, (1, 5))
                near = (send(ours, first_perm), send(cross, cross_perm))
                other = send(tensor.extract(owners, grad, (4, 6)), core_perm)
                turn = send(tensor.pair_sum(owners, grad, other, 2, 1, None, far), second_perm)
                new_m, new_v, dirn, sums = tensor.moments(owners, grad, other, None, turn, *state, near)
            else:
                other_far = send(tensor.extract(owners, grad, (7,)), core_perm)
                other = send(tensor.extract(owners, grad, (4, 5, 6)), core_perm)
                far = send(tensor.pair_sum(owners, grad, other_far, 3, 0), first_perm)
                near = send(tensor.pair_sum(owners, grad, other, 1, 1), first_perm)
                turn = send(tensor.pair_sum(owners, grad, other, 2, 2, far), second_perm)
                new_m, new_v, dirn, sums = tensor.moments(owners, grad, other, near, turn, *state)
            sums = sums + send(sums, core_perm)
            sums = (sums + send(sums, both_perm)) + (send(sums, first_perm) + send(sums, second_perm))
            new_w, packed = copies.apply(owners, sums, weight, dirn)
            by_second = send(packed, second_perm)
            by_first = send(packed, first_perm)
            by_both = send(by_second, first_perm)
            whole = None
            for owner, part in ((0, packed), (2, by_second), (1, by_first), (3, by_both)):
                theirs = send(part, core_perm)
                whole = copies.unpack(owners, owner, part, theirs, whole)
            results.extend((whole, new_w, new_m, new_v))
        return tuple(results)

    return jax.shard_map(
        device_step,
        mesh=mesh,
        in_specs=(grad_spec, shard_spec, shard_spec, shard_spec) * 4,
        out_specs=(full_spec, shard_spec, shard_spec, shard_spec) * 4,
        check_vma=False,
    )
```
